16 devices in a mesh: tp: 16 (over z, y, x, core).
Axes of the slice: x: 2, y: 2, z: 2, core: 2. Of those that a mesh axis runs over, the one named last changes fastest.
Arguments:
- tokens: int32 [2, 128], replicated
- lengths: int32 [128], replicated
- embedding: bfloat16 [51200, 2560], P('tp')
- ln_scale: float32 [2, 2560], replicated
- w_q: bfloat16 [2, 2560, 32, 80], P(None, None, 'tp')
- w_kv: bfloat16 [2, 2560, 160], replicated
- w_o: bfloat16 [2, 32, 80, 2560], P(None, 'tp')
- w_gate: bfloat16 [2, 2560, 10240], P(None, None, 'tp')
- w_up: bfloat16 [2, 2560, 10240], P(None, None, 'tp')
- w_down: bfloat16 [2, 10240, 2560], P(None, 'tp')
- final_scale: float32 [2560], replicated
- k_cache: bfloat16 [2, 128, 2048, 80], P(None, 'tp')
- v_cache: bfloat16 [2, 128, 2048, 80], P(None, 'tp')
Outputs:
- output 1: float32 [2, 128, 51200], P(None, None, 'tp')
- output 2: bfloat16 [2, 128, 2048, 80], P(None, 'tp')
- output 3: bfloat16 [2, 128, 2048, 80], P(None, 'tp')
All inputs are finite; a program needn't handle non-finite values.
Results may differ from the reference program's by a relative error of at most 0.00684216.
Values are sent between devices in bfloat16 or wider.
A program may use at most 1 GiB of HBM per device.

```python
import jax
import jax.numpy as jnp
from jax import lax

VOCAB = 51200
D = 2560
HEADS = 32
HEAD = 80
FF = 10240
BATCH = 128
SEQ = 2048
STEPS = 2
LAYERS = 2
LN_EPS = 1e-6


def draw_tokens(rng_key):
    key_off, key_perm = jax.random.split(rng_key)
    stride = VOCAB // BATCH
    starts = (jnp.arange(BATCH, dtype=jnp.int32) * VOCAB) // BATCH
    offsets = jax.random.randint(key_off, (STEPS, BATCH), 0, stride, dtype=jnp.int32)
    orders = jax.vmap(lambda one_key: jax.random.permutation(one_key, BATCH))(jax.random.split(key_perm, STEPS))
    return jnp.take_along_axis(starts[None, :] + offsets, orders, axis=1)


def draw_lengths(rng_key):
    key_base, key_shift, key_pick = jax.random.split(rng_key, 3)
    longest = SEQ - STEPS
    base_len = jax.random.randint(key_base, (BATCH,), 1, longest + 1, dtype=jnp.int32)
    shifts = jax.random.randint(key_shift, (BATCH,), 0, 8, dtype=jnp.int32)
    short_len = jnp.maximum(jnp.right_shift(base_len, shifts), 1)
    chosen = jax.random.randint(key_pick, (), 0, BATCH, dtype=jnp.int32)
    return jnp.where(jnp.arange(BATCH, dtype=jnp.int32) == chosen, longest, short_len).astype(jnp.int32)


def normal_draw(rng_key, arr_shape, spread):
    return jax.random.normal(rng_key, arr_shape, jnp.float32) * spread


def setup_inputs(seed: int = 0) -> dict:
    key_list = jax.random.split(jax.random.key(seed), 14)
    cache_shape = (LAYERS, BATCH, SEQ, HEAD)
    return {
        'tokens': draw_tokens(key_list[0]),
        'lengths': draw_lengths(key_list[1]),
        'embedding': normal_draw(key_list[2], (VOCAB, D), 1.0).astype(jnp.bfloat16),
        'ln_scale': 1.0 + normal_draw(key_list[3], (LAYERS, D), 0.2),
        'w_q': normal_draw(key_list[4], (LAYERS, D, HEADS, HEAD), D ** -0.5).astype(jnp.bfloat16),
        'w_kv': normal_draw(key_list[5], (LAYERS, D, 2 * HEAD), D ** -0.5).astype(jnp.bfloat16),
        'w_o': normal_draw(key_list[6], (LAYERS, HEADS, HEAD, D), (HEADS * HEAD) ** -0.5).astype(jnp.bfloat16),
        'w_gate': normal_draw(key_list[7], (LAYERS, D, FF), D ** -0.5).astype(jnp.bfloat16),
        'w_up': normal_draw(key_list[8], (LAYERS, D, FF), D ** -0.5).astype(jnp.bfloat16),
        'w_down': normal_draw(key_list[9], (LAYERS, FF, D), FF ** -0.5).astype(jnp.bfloat16),
        'final_scale': 1.0 + normal_draw(key_list[10], (D,), 0.2),
        'k_cache': normal_draw(key_list[11], cache_shape, 1.5).astype(jnp.bfloat16),
        'v_cache': (normal_draw(key_list[12], cache_shape, 1.0) + normal_draw(key_list[13], (LAYERS, BATCH, 1, HEAD), 0.7)).astype(jnp.bfloat16),
    }


def layer_norm(residual, ln_gain):
    x_f32 = residual.astype(jnp.float32)
    row_mean = jnp.mean(x_f32, axis=-1, keepdims=True)
    centred = x_f32 - row_mean
    row_var = jnp.mean(centred * centred, axis=-1, keepdims=True)
    return (centred * lax.rsqrt(row_var + LN_EPS) * ln_gain).astype(jnp.bfloat16)


def rotary(features, positions):
    half_dim = features.shape[-1] // 2
    inv_freq = 10000.0 ** (-jnp.arange(half_dim, dtype=jnp.float32) / half_dim)
    angles = positions[..., None].astype(jnp.float32) * inv_freq
    cos_t = jnp.cos(angles)
    sin_t = jnp.sin(angles)
    lo_half = features[..., :half_dim]
    hi_half = features[..., half_dim:]
    return jnp.concatenate([lo_half * cos_t - hi_half * sin_t, lo_half * sin_t + hi_half * cos_t], axis=-1)


def attend_one(operands):
    query_rows, keys_seq, values_seq, position = operands
    scores = jnp.dot(query_rows, keys_seq.T, preferred_element_type=jnp.float32) * HEAD ** -0.5
    visible = jnp.arange(SEQ) <= position
    scores = jnp.where(visible[None, :], scores, -jnp.inf)
    attn_probs = jax.nn.softmax(scores, axis=-1).astype(jnp.bfloat16)
    return jnp.dot(attn_probs, values_seq, preferred_element_type=jnp.float32).astype(jnp.bfloat16)


def decode_layer(residual, positions, layer_params):
    ln_gain, w_q, w_kv, w_o, w_gate, w_up, w_down, k_layer, v_layer = layer_params
    normed = layer_norm(residual, ln_gain)
    q_flat = jnp.dot(normed, w_q.reshape(D, HEADS * HEAD), preferred_element_type=jnp.float32)
    queries = rotary(q_flat.reshape(BATCH, HEADS, HEAD), positions[:, None]).astype(jnp.bfloat16)
    kv_new = jnp.dot(normed, w_kv, preferred_element_type=jnp.float32)
    k_new = rotary(kv_new[:, :HEAD], positions).astype(jnp.bfloat16)
    v_new = kv_new[:, HEAD:].astype(jnp.bfloat16)
    batch_idx = jnp.arange(BATCH)
    k_layer = k_layer.at[batch_idx, positions].set(k_new)
    v_layer = v_layer.at[batch_idx, positions].set(v_new)
    attn_out = lax.map(attend_one, (queries, k_layer, v_layer, positions))
    attn_sum = jnp.dot(attn_out.reshape(BATCH, HEADS * HEAD), w_o.reshape(HEADS * HEAD, D), preferred_element_type=jnp.float32)
    gate_proj = jnp.dot(normed, w_gate, preferred_element_type=jnp.float32)
    up_proj = jnp.dot(normed, w_up, preferred_element_type=jnp.float32)
    hidden = (jax.nn.silu(gate_proj) * up_proj).astype(jnp.bfloat16)
    mlp_sum = jnp.dot(hidden, w_down, preferred_element_type=jnp.float32)
    residual = (residual.astype(jnp.float32) + (attn_sum + mlp_sum)).astype(jnp.bfloat16)
    return residual, k_layer, v_layer


def reference(tokens, lengths, embedding, ln_scale, w_q, w_kv, w_o, w_gate, w_up, w_down, final_scale, k_cache, v_cache):
    def one_step(caches, step_in):
        k_all, v_all = caches
        tok_row, step_idx = step_in
        positions = lengths + step_idx
        residual = embedding[tok_row]

        def one_layer(resid_in, layer_params):
            resid_out, k_layer, v_layer = decode_layer(resid_in, positions, layer_params)
            return resid_out, (k_layer, v_layer)

        residual, (k_all, v_all) = lax.scan(one_layer, residual, (ln_scale, w_q, w_kv, w_o, w_gate, w_up, w_down, k_all, v_all))
        normed = layer_norm(residual, final_scale)
        logits = jnp.dot(normed, embedding.T, preferred_element_type=jnp.float32) * D ** -0.5
        return (k_all, v_all), logits

    (k_out, v_out), logits = lax.scan(one_step, (k_cache, v_cache), (tokens, jnp.arange(STEPS, dtype=jnp.int32)))
    return logits, k_out, v_out
```

```python
import functools

import jax
import jax.numpy as jnp
from jax import lax
from jax.experimental import pallas as pl
from jax.experimental.pallas import tpu as pltpu
from jax.sharding import PartitionSpec as P

LN_EPS = 1e-6
F32 = jnp.float32
BF16 = jnp.bfloat16


def layer_norm(residual, ln_gain):
    x_f32 = residual.astype(F32)
    row_mean = jnp.mean(x_f32, axis=-1, keepdims=True)
    centred = x_f32 - row_mean
    row_var = jnp.mean(centred * centred, axis=-1, keepdims=True)
    return (centred * lax.rsqrt(row_var + LN_EPS) * ln_gain).astype(BF16)


def attn_kernel(layer, has_alias, steps, seqs, len_ref, q_ref, kn_ref, vn_ref, kc_ref, vc_ref, *rest):
    if has_alias:
        rest = rest[2:]
    o_ref, ko_ref, vo_ref, kbuf, vbuf, qa, qb, oa, ob, isem, osem = rest
    head_dim, seq_len = kbuf.shape[1], kbuf.shape[2]
    rows_per = steps * seqs
    srcs = q_ref.shape[0] // rows_per
    width2 = q_ref.shape[1]

    def in_copies(s):
        return (pltpu.make_async_copy(kc_ref.at[layer, s], kbuf.at[s], isem.at[0, s]),
                pltpu.make_async_copy(vc_ref.at[layer, s], vbuf.at[s], isem.at[1, s]))

    def out_copies(s):
        return (pltpu.make_async_copy(kbuf.at[s], ko_ref.at[layer, s], osem.at[0, s]),
                pltpu.make_async_copy(vbuf.at[s], vo_ref.at[layer, s], osem.at[1, s]))

    for s in range(seqs):
        for cp in in_copies(s):
            cp.start()
    qa[...] = q_ref[:, :128].astype(F32)
    qb[...] = jnp.zeros_like(qb)
    qb[:, :width2 - 128] = q_ref[:, 128:].astype(F32)
    lane = lax.broadcasted_iota(jnp.int32, (head_dim, 128), 1)
    for s in range(seqs):
        for cp in in_copies(s):
            cp.wait()
        for t in range(steps):
            p = len_ref[s] + t
            base = pl.multiple_of((p // 128) * 128, 128)
            hit = lane == (p - base)
            c = t * seqs + s
            for buf, new in ((kbuf, kn_ref), (vbuf, vn_ref)):
                tile = buf[s, :, pl.ds(base, 128)].astype(F32)
                buf[s, :, pl.ds(base, 128)] = jnp.where(hit, new[:, c:c + 1], tile).astype(BF16)
        for cp in out_copies(s):
            cp.start()

    half = lax.broadcasted_iota(jnp.int32, (steps * srcs, width2), 1) < head_dim
    n_rows = 2 * steps * srcs
    scale = head_dim ** -0.5

    def attend(s, width):
        p = len_ref[s]
        at = [pl.ds(t * seqs + s, srcs, stride=rows_per) for t in range(steps)]
        qcat = jnp.concatenate([jnp.concatenate([qa[i, :], qb[i, :]], axis=1)[:, :width2] for i in at], axis=0)
        q2 = jnp.concatenate([jnp.where(half, qcat, 0.0), jnp.where(half, 0.0, qcat)], axis=0).astype(BF16)
        k = kbuf[s, :, 0:width]
        k2 = jnp.concatenate([k, k], axis=0)
        sc = jnp.dot(q2, k2, preferred_element_type=F32) * scale
        row = lax.broadcasted_iota(jnp.int32, (n_rows, width), 0)
        col = lax.broadcasted_iota(jnp.int32, (n_rows, width), 1)
        lim = p + lax.rem(row // srcs, steps)
        sc = jnp.where(col <= lim, sc, -jnp.inf)
        m = jnp.max(sc, axis=-1, keepdims=True)
        e = jnp.exp(sc - m)
        w = (e / jnp.sum(e, axis=-1, keepdims=True)).astype(BF16)
        v = vbuf[s, :, 0:width]
        v2 = jnp.concatenate([v, v], axis=0)
        o2 = lax.dot_general(w, v2, (((1,), (1,)), ((), ())), preferred_element_type=F32)
        o = jnp.where(half, o2[:n_rows // 2], o2[n_rows // 2:])
        o = jnp.concatenate([o, jnp.zeros((steps * srcs, 256 - width2), F32)], axis=1)
        for t in range(steps):
            oa[at[t], :] = o[t * srcs:(t + 1) * srcs, :128]
            ob[at[t], :] = o[t * srcs:(t + 1) * srcs, 128:]

    widths = [w for w in (256, 512, 1024) if w < seq_len] + [seq_len]

    @pl.loop(0, seqs)
    def _(s):
        last = len_ref[s] + (steps - 1)
        lo = 0
        for w in widths:
            @pl.when((last >= lo) & (last < w))
            def _():
                attend(s, w)
            lo = w

    o_ref[:, :128] = oa[...].astype(BF16)
    o_ref[:, 128:] = ob[:, :width2 - 128].astype(BF16)
    for s in range(seqs):
        for cp in out_copies(s):
            cp.wait()


def attention(layer, steps, local_len, q, k_new, v_new, kc, vc, outs):
    layers, seqs, head_dim, seq_len = kc.shape
    rows, width = q.shape
    any_spec = pl.BlockSpec(memory_space=pl.ANY)
    vm = pl.BlockSpec(memory_space=pltpu.VMEM)
    args = [local_len, q, k_new, v_new, kc, vc]
    in_specs = [pl.BlockSpec(memory_space=pltpu.SMEM), vm, vm, vm, any_spec, any_spec]
    aliases = {}
    if outs is not None:
        args += list(outs)
        in_specs += [any_spec, any_spec]
        aliases = {6: 1, 7: 2}
    return pl.pallas_call(
        functools.partial(attn_kernel, layer, outs is not None, steps, seqs),
        out_shape=(jax.ShapeDtypeStruct((rows, width), BF16), jax.ShapeDtypeStruct(kc.shape, BF16), jax.ShapeDtypeStruct(vc.shape, BF16)),
        in_specs=in_specs,
        out_specs=(vm, any_spec, any_spec),
        scratch_shapes=[
            pltpu.VMEM((seqs, head_dim, seq_len), BF16),
            pltpu.VMEM((seqs, head_dim, seq_len), BF16),
            pltpu.VMEM((rows, 128), F32),
            pltpu.VMEM((rows, 128), F32),
            pltpu.VMEM((rows, 128), F32),
            pltpu.VMEM((rows, 128), F32),
            pltpu.SemaphoreType.DMA((2, seqs)),
            pltpu.SemaphoreType.DMA((2, seqs)),
        ],
        input_output_aliases=aliases,
        compiler_params=pltpu.CompilerParams(vmem_limit_bytes=24 << 20),
        cost_estimate=pl.CostEstimate(flops=2_000_000_000, bytes_accessed=21 << 20, transcendentals=1 << 20),
        name=f"attend{layer}",
    )(*args)


def solution(mesh):
    n_dev = mesh.size

    def device_fn(tokens, lengths, embedding, ln_scale, w_q, w_kv, w_o, w_gate, w_up, w_down, final_scale, k_cache, v_cache):
        rank = lax.axis_index('tp')
        steps, batch = tokens.shape
        vocab_local, dim = embedding.shape
        layers, seqs, seq_len, head_dim = k_cache.shape
        heads_local = w_q.shape[2]
        width = heads_local * head_dim
        rows = steps * batch
        half = head_dim // 2
        kc = jnp.swapaxes(k_cache, 2, 3)
        vc = jnp.swapaxes(v_cache, 2, 3)
        local_len = lax.dynamic_slice_in_dim(lengths, rank * seqs, seqs)

        def by_device(per_step):
            return per_step.reshape(steps, n_dev, seqs).transpose(1, 0, 2).reshape(rows)

        tok = by_device(tokens)
        positions = by_device(lengths[None, :] + jnp.arange(steps, dtype=jnp.int32)[:, None])
        inv_freq = 10000.0 ** (-jnp.arange(half, dtype=F32) / half)
        ang = positions[:, None].astype(F32) * inv_freq
        cos_t = jnp.cos(ang)
        sin_t = jnp.sin(ang)
        cos_q = jnp.tile(cos_t, (1, 2 * heads_local))
        sin_q = jnp.tile(jnp.concatenate([-sin_t, sin_t], axis=1), (1, heads_local))
        local_rows = steps * seqs
        cos_k = lax.dynamic_slice_in_dim(cos_t, rank * local_rows, local_rows).T
        sin_k = lax.dynamic_slice_in_dim(sin_t, rank * local_rows, local_rows).T

        onehot = (tok[:, None] - rank * vocab_local == jnp.arange(vocab_local, dtype=jnp.int32)[None, :]).astype(BF16)
        emb = jnp.dot(onehot, embedding, preferred_element_type=F32).astype(BF16)
        x = lax.psum_scatter(emb, 'tp', scatter_dimension=0, tiled=True)
        outs = None
        for l in range(layers):
            h_local = layer_norm(x, ln_scale[l])
            h = lax.all_gather(h_local, 'tp', axis=0, tiled=True)
            q = jnp.dot(h, w_q[l].reshape(dim, width), preferred_element_type=F32)
            q4 = q.reshape(rows, heads_local, 2, half)
            q_sw = q4[:, :, ::-1].reshape(rows, width)
            q = (q * cos_q + q_sw * sin_q).astype(BF16)
            kv = lax.dot_general(w_kv[l], h_local, (((0,), (1,)), ((), ())), preferred_element_type=F32)
            k_lo, k_hi, v_new = kv[:half], kv[half:head_dim], kv[head_dim:]
            k_new = jnp.concatenate([k_lo * cos_k - k_hi * sin_k, k_lo * sin_k + k_hi * cos_k], axis=0)
            k_new = lax.reduce_precision(k_new, 8, 7)
            v_new = lax.reduce_precision(v_new, 8, 7)
            q_seq = lax.all_to_all(q, 'tp', 0, 0, tiled=True)
            o, *outs = attention(l, steps, local_len, q_seq, k_new, v_new, kc, vc, outs)
            gate = jnp.dot(h, w_gate[l], preferred_element_type=F32)
            up = jnp.dot(h, w_up[l], preferred_element_type=F32)
            hidden = (jax.nn.silu(gate) * up).astype(BF16)
            mlp = jnp.dot(hidden, w_down[l], preferred_element_type=F32)
            o_heads = lax.all_to_all(o, 'tp', 0, 0, tiled=True)
            part = jnp.dot(o_heads, w_o[l].reshape(width, dim), preferred_element_type=F32) + mlp
            total = lax.psum_scatter(part, 'tp', scatter_dimension=0, tiled=True)
            x = (x.astype(F32) + total).astype(BF16)
        h_local = layer_norm(x, final_scale)
        h = lax.all_gather(h_local, 'tp', axis=0, tiled=True)
        logits = lax.dot_general(h, embedding, (((1,), (1,)), ((), ())), preferred_element_type=F32) * dim ** -0.5
        logits = logits.reshape(n_dev, steps, seqs, vocab_local).transpose(1, 0, 2, 3).reshape(steps, batch, vocab_local)
        k_out, v_out = outs
        return logits, jnp.swapaxes(k_out, 2, 3), jnp.swapaxes(v_out, 2, 3)

    cache_spec = P(None, 'tp', None, None)
    in_specs = (P(), P(), P('tp', None), P(), P(None, None, 'tp', None), P(), P(None, 'tp', None, None), P(None, None, 'tp'), P(None, None, 'tp'), P(None, 'tp', None), P(), cache_spec, cache_spec)
    out_specs = (P(None, None, 'tp'), cache_spec, cache_spec)
    return jax.shard_map(device_fn, mesh=mesh, in_specs=in_specs, out_specs=out_specs, check_vma=False)
```

```python
import functools

import jax
import jax.numpy as jnp
from jax import lax
from jax.experimental import pallas as pl
from jax.experimental.pallas import tpu as pltpu
from jax.sharding import PartitionSpec as P

LN_EPS = 1e-6
F32 = jnp.float32
BF16 = jnp.bfloat16


def attn_kernel(layer, has_alias, steps, seqs, len_ref, q_ref, kn_ref, vn_ref, kc_ref, vc_ref, *rest):
    if has_alias:
        rest = rest[2:]
    o_ref, ko_ref, vo_ref, kbuf, vbuf, qa, qb, oa, ob, isem, osem = rest
    head_dim, seq_len = kbuf.shape[1], kbuf.shape[2]
    rows_per = steps * seqs
    srcs = q_ref.shape[0] // rows_per
    width2 = q_ref.shape[1]

    def in_copies(s):
        return (pltpu.make_async_copy(kc_ref.at[layer, s], kbuf.at[s], isem.at[0, s]),
                pltpu.make_async_copy(vc_ref.at[layer, s], vbuf.at[s], isem.at[1, s]))

    def out_copies(s):
        return (pltpu.make_async_copy(kbuf.at[s], ko_ref.at[layer, s], osem.at[0, s]),
                pltpu.make_async_copy(vbuf.at[s], vo_ref.at[layer, s], osem.at[1, s]))

    for s in range(seqs):
        for cp in in_copies(s):
            cp.start()
    qa[...] = q_ref[:, :128].astype(F32)
    qb[...] = jnp.zeros_like(qb)
    qb[:, :width2 - 128] = q_ref[:, 128:].astype(F32)
    lane = lax.broadcasted_iota(jnp.int32, (head_dim, 128), 1)
    for s in range(seqs):
        for cp in in_copies(s):
            cp.wait()
        for t in range(steps):
            p = len_ref[s] + t
            base = pl.multiple_of((p // 128) * 128, 128)
            hit = lane == (p - base)
            c = t * seqs + s
            for buf, new in ((kbuf, kn_ref), (vbuf, vn_ref)):
                tile = buf[s, :, pl.ds(base, 128)].astype(F32)
                buf[s, :, pl.ds(base, 128)] = jnp.where(hit, new[:, c:c + 1], tile).astype(BF16)
        for cp in out_copies(s):
            cp.start()

    half = lax.broadcasted_iota(jnp.int32, (steps * srcs, width2), 1) < head_dim
    n_rows = 2 * steps * srcs
    scale = head_dim ** -0.5

    def attend(s, width):
        p = len_ref[s]
        at = [pl.ds(t * seqs + s, srcs, stride=rows_per) for t in range(steps)]
        qcat = jnp.concatenate([jnp.concatenate([qa[i, :], qb[i, :]], axis=1)[:, :width2] for i in at], axis=0)
        q2 = jnp.concatenate([jnp.where(half, qcat, 0.0), jnp.where(half, 0.0, qcat)], axis=0).astype(BF16)
        k = kbuf[s, :, 0:width]
        k2 = jnp.concatenate([k, k], axis=0)
        sc = jnp.dot(q2, k2, preferred_element_type=F32) * scale
        row = lax.broadcasted_iota(jnp.int32, (n_rows, width), 0)
        col = lax.broadcasted_iota(jnp.int32, (n_rows, width), 1)
        lim = p + lax.rem(row // srcs, steps)
        sc = jnp.where(col <= lim, sc, -jnp.inf)
        m = jnp.max(sc, axis=-1, keepdims=True)
        e = jnp.exp(sc - m)
        w = (e / jnp.sum(e, axis=-1, keepdims=True)).astype(BF16)
        v = vbuf[s, :, 0:width]
        v2 = jnp.concatenate([v, v], axis=0)
        o2 = lax.dot_general(w, v2, (((1,), (1,)), ((), ())), preferred_element_type=F32)
        o = jnp.where(half, o2[:n_rows // 2], o2[n_rows // 2:])
        o = jnp.concatenate([o, jnp.zeros((steps * srcs, 256 - width2), F32)], axis=1)
        for t in range(steps):
            oa[at[t], :] = o[t * srcs:(t + 1) * srcs, :128]
            ob[at[t], :] = o[t * srcs:(t + 1) * srcs, 128:]

    widths = [w for w in (256, 512, 1024) if w < seq_len] + [seq_len]

    @pl.loop(0, seqs)
    def _(s):
        last = len_ref[s] + (steps - 1)
        lo = 0
        for w in widths:
            @pl.when((last >= lo) & (last < w))
            def _():
                attend(s, w)
            lo = w

    o_ref[:, :128] = oa[...].astype(BF16)
    o_ref[:, 128:] = ob[:, :width2 - 128].astype(BF16)
    for s in range(seqs):
        for cp in out_copies(s):
            cp.wait()


def attention(layer, steps, local_len, q, k_new, v_new, kc, vc, outs):
    layers, seqs, head_dim, seq_len = kc.shape
    rows, width = q.shape
    any_spec = pl.BlockSpec(memory_space=pltpu.HBM)
    vm = pl.BlockSpec(memory_space=pltpu.VMEM)
    args = [local_len, q, k_new, v_new, kc, vc]
    in_specs = [pl.BlockSpec(memory_space=pltpu.SMEM), vm, vm, vm, any_spec, any_spec]
    aliases = {}
    if outs is not None:
        args += list(outs)
        in_specs += [any_spec, any_spec]
        aliases = {6: 1, 7: 2}
    return pl.pallas_call(
        functools.partial(attn_kernel, layer, outs is not None, steps, seqs),
        out_shape=(jax.ShapeDtypeStruct((rows, width), BF16), jax.ShapeDtypeStruct(kc.shape, BF16), jax.ShapeDtypeStruct(vc.shape, BF16)),
        in_specs=in_specs,
        out_specs=(vm, any_spec, any_spec),
        scratch_shapes=[
            pltpu.VMEM((seqs, head_dim, seq_len), BF16),
            pltpu.VMEM((seqs, head_dim, seq_len), BF16),
            pltpu.VMEM((rows, 128), F32),
            pltpu.VMEM((rows, 128), F32),
            pltpu.VMEM((rows, 128), F32),
            pltpu.VMEM((rows, 128), F32),
            pltpu.SemaphoreType.DMA((2, seqs)),
            pltpu.SemaphoreType.DMA((2, seqs)),
        ],
        input_output_aliases=aliases,
        compiler_params=pltpu.CompilerParams(vmem_limit_bytes=24 << 20),
        cost_estimate=pl.CostEstimate(flops=2_000_000_000, bytes_accessed=21 << 20, transcendentals=1 << 20),
        name=f"attend{layer}",
    )(*args)


def device(d):
    return {"device_id": (d,), "device_id_type": pl.DeviceIdType.MESH}


def enter(n_dev, me):
    sem = pltpu.get_barrier_semaphore()
    for i in range(1, n_dev):
        pl.semaphore_signal(sem, inc=1, **device(lax.rem(me + i, n_dev)))
    return sem


def chip_at(chip, j, n_bits):
    total = 0
    for i in range(n_bits):
        total = total + lax.rem(chip // (1 << i) + ((j >> i) & 1), 2) * (1 << i)
    return total


def block(d, rows):
    return pl.ds(pl.multiple_of(d * rows, rows), rows)


def norm_rows(x_f32, gain):
    row_mean = jnp.mean(x_f32, axis=-1, keepdims=True)
    centred = x_f32 - row_mean
    row_var = jnp.mean(centred * centred, axis=-1, keepdims=True)
    return (centred * lax.rsqrt(row_var + LN_EPS) * gain).astype(BF16)


def reduce_gather(n_dev, me, part, x_ref, gain, x_out, h_out, hloc, d2d, stage, rem, sems, while_gathering):
    d2d_s, d2d_r, far_s, far_r, ag_s, ag_r, fw_s, fw_r = sems
    n_chips = n_dev // 2
    n_bits = n_chips.bit_length() - 1
    rows = hloc.shape[0]
    chip, core = me // 2, lax.rem(me, 2)
    sibling = chip * 2 + 1 - core
    order = sorted(range(n_chips), key=lambda j: -bin(j).count("1"))

    def pre(j):
        c = chip_at(chip, j, n_bits)
        return pltpu.make_async_remote_copy(part.at[block(c * 2 + 1 - core, rows)], d2d.at[j], d2d_s.at[j], d2d_r.at[j], **device(sibling))

    def far(j):
        c = chip_at(chip, j, n_bits)
        return pltpu.make_async_remote_copy(stage.at[j], rem.at[j], far_s.at[j], far_r.at[j], **device(c * 2 + core))

    for j in order:
        pre(j).start()
    for j in order[:-1]:
        pre(j).wait_recv()
        c = chip_at(chip, j, n_bits)
        stage[j] = (part[block(c * 2 + core, rows)].astype(F32) + d2d[j].astype(F32)).astype(stage.dtype)
        far(j).start()
    pre(0).wait_recv()
    acc = part[block(me, rows)].astype(F32) + d2d[0].astype(F32)
    for j in reversed(order[:-1]):
        far(j).wait_recv()
        acc = acc + rem[j].astype(F32)
    if x_ref is not None:
        acc = x_ref[...].astype(F32) + acc
    x_new = acc.astype(BF16)
    x_out[...] = x_new
    hloc[...] = norm_rows(x_new.astype(F32), gain)
    h_out[block(me, rows)] = hloc[...]

    def gather(j):
        c = chip_at(chip, j, n_bits)
        return pltpu.make_async_remote_copy(hloc, h_out.at[block(me, rows)], ag_s.at[j], ag_r.at[j], **device(c * 2 + core if j else sibling))

    def relay(j):
        c = chip_at(chip, j, n_bits)
        blk = h_out.at[block(c * 2 + core, rows)]
        return pltpu.make_async_remote_copy(blk, blk, fw_s.at[j], fw_r.at[j], **device(sibling))

    for j in order:
        gather(j).start()
    while_gathering()
    for j in reversed(order[:-1]):
        gather(j).wait_recv()
        relay(j).start()
    gather(0).wait_recv()
    for j in order[:-1]:
        relay(j).wait_recv()
    for j in order:
        pre(j).wait_send()
        gather(j).wait_send()
        if j:
            far(j).wait_send()
            relay(j).wait_send()


def project_kv(hloc, wkv_ref, cos_ref, sin_ref, kn_ref, vn_ref):
    head_dim = kn_ref.shape[0]
    half = head_dim // 2
    kv = lax.dot_general(wkv_ref[...], hloc[...], (((1,), (1,)), ((), ())), preferred_element_type=F32)
    k_lo, k_hi = kv[:half], kv[half:head_dim]
    cos, sin = cos_ref[...], sin_ref[...]
    kn_ref[...] = jnp.concatenate([k_lo * cos - k_hi * sin, k_lo * sin + k_hi * cos], axis=0).astype(BF16).astype(F32)
    vn_ref[...] = kv[head_dim:].astype(BF16).astype(F32)


def reduce_scratch(n_dev, rows, dim, dtype):
    n_chips = n_dev // 2
    return [pltpu.VMEM((rows, dim), BF16)] + [pltpu.VMEM((n_chips, rows, dim), dtype)] * 3 + [pltpu.SemaphoreType.DMA((n_chips,))] * 8


def boundary_kernel(n_dev, kind, last, *refs):
    refs = list(refs)
    take = lambda n: [refs.pop(0) for _ in range(n)]
    if kind == "embed":
        part_in, gain = take(2)
        x_ref = None
    else:
        o_ref, wo_ref, mlp_ref, x_ref, gain = take(5)
    if not last:
        wkv_ref, cos_ref, sin_ref = take(3)
    x_out, h_out = take(2)
    if not last:
        kn_ref, vn_ref = take(2)
    if kind == "embed":
        part = part_in
    else:
        heads, part, a2a_s, a2a_r = take(4)
    hloc, d2d, stage, rem, *sems = refs
    me = lax.axis_index("tp")
    bar = enter(n_dev, me)
    pl.semaphore_wait(bar, n_dev - 1)
    rows = hloc.shape[0]
    if kind != "embed":
        def send(i):
            d = lax.rem(me + i, n_dev)
            return pltpu.make_async_remote_copy(o_ref.at[block(d, rows)], heads.at[block(me, rows)], a2a_s.at[i], a2a_r.at[i], **device(d))
        for i in range(1, n_dev):
            send(i).start()
        heads[block(me, rows)] = o_ref[block(me, rows)]
        for i in range(1, n_dev):
            send(i).wait_recv()
        part[...] = jnp.dot(heads[...], wo_ref[...], preferred_element_type=F32) + mlp_ref[...]
    body = (lambda: None) if last else (lambda: project_kv(hloc, wkv_ref, cos_ref, sin_ref, kn_ref, vn_ref))
    reduce_gather(n_dev, me, part, x_ref, gain[...], x_out, h_out, hloc, d2d, stage, rem, sems, body)
    if kind != "embed":
        for i in range(1, n_dev):
            send(i).wait_send()


def boundary(n_dev, kind, index, ins, gain, kv_ins, rows_total):
    vm = pl.BlockSpec(memory_space=pltpu.VMEM)
    dim = gain.shape[1]
    rows = rows_total // n_dev
    last = kv_ins is None
    args = list(ins) + [gain] + ([] if last else list(kv_ins))
    out_shape = [jax.ShapeDtypeStruct((rows, dim), BF16), jax.ShapeDtypeStruct((rows_total, dim), BF16)]
    if not last:
        head_dim = kv_ins[0].shape[0] // 2
        out_shape += [jax.ShapeDtypeStruct((head_dim, rows), F32)] * 2
    scratch = []
    if kind != "embed":
        width = ins[0].shape[1]
        scratch = [pltpu.VMEM((rows_total, width), BF16), pltpu.VMEM((rows_total, dim), F32), pltpu.SemaphoreType.DMA((n_dev,)), pltpu.SemaphoreType.DMA((n_dev,))]
    scratch += reduce_scratch(n_dev, rows, dim, BF16 if kind == "embed" else F32)
    return pl.pallas_call(
        functools.partial(boundary_kernel, n_dev, kind, last),
        out_shape=tuple(out_shape),
        in_specs=[vm] * len(args),
        out_specs=tuple([vm] * len(out_shape)),
        scratch_shapes=scratch,
        compiler_params=pltpu.CompilerParams(vmem_limit_bytes=24 << 20, collective_id=index, has_side_effects=True),
        cost_estimate=pl.CostEstimate(flops=20_000_000_000, bytes_accessed=8 << 20, transcendentals=0),
        name=f"boundary{index}",
    )(*args)


def project_kernel(n_dev, h_ref, wq_ref, cos_ref, sin_ref, wg_ref, wu_ref, wd_ref, q_out, mlp_ref, q_buf, hid, s_sem, r_sem):
    me = lax.axis_index("tp")
    bar = enter(n_dev, me)
    rows = q_buf.shape[0] // n_dev
    half = cos_ref.shape[0]
    h = h_ref[...]
    qt = lax.dot_general(wq_ref[...], h, (((1,), (1,)), ((), ())), preferred_element_type=F32)
    cos, sin = cos_ref[...], sin_ref[...]
    parts = []
    for a in range(0, qt.shape[0], 2 * half):
        lo, hi = qt[a:a + half], qt[a + half:a + 2 * half]
        parts += [lo * cos - hi * sin, lo * sin + hi * cos]
    q_buf[...] = jnp.concatenate(parts, axis=0).T.astype(BF16)
    pl.semaphore_wait(bar, n_dev - 1)

    def send(i):
        d = lax.rem(me + i, n_dev)
        return pltpu.make_async_remote_copy(q_buf.at[block(d, rows)], q_out.at[block(me, rows)], s_sem.at[i], r_sem.at[i], **device(d))

    for i in range(1, n_dev):
        send(i).start()
    q_out[block(me, rows)] = q_buf[block(me, rows)]
    gate = jnp.dot(h, wg_ref[...], preferred_element_type=F32)
    up = jnp.dot(h, wu_ref[...], preferred_element_type=F32)
    hid[...] = (gate * jax.nn.sigmoid(gate) * up).astype(BF16)
    mlp_ref[...] = jnp.dot(hid[...], wd_ref[...], preferred_element_type=F32)
    for i in range(1, n_dev):
        send(i).wait_recv()
    for i in range(1, n_dev):
        send(i).wait_send()


def project(n_dev, index, h, wq_t, cos_t, sin_t, wg, wu, wd):
    vm = pl.BlockSpec(memory_space=pltpu.VMEM)
    rows, dim = h.shape
    width = wq_t.shape[0]
    return pl.pallas_call(
        functools.partial(project_kernel, n_dev),
        out_shape=(jax.ShapeDtypeStruct((rows, width), BF16), jax.ShapeDtypeStruct((rows, dim), F32)),
        in_specs=[vm] * 7,
        out_specs=(vm, vm),
        scratch_shapes=[pltpu.VMEM((rows, width), BF16), pltpu.VMEM((rows, wg.shape[1]), BF16), pltpu.SemaphoreType.DMA((n_dev,)), pltpu.SemaphoreType.DMA((n_dev,))],
        compiler_params=pltpu.CompilerParams(vmem_limit_bytes=28 << 20, collective_id=index, has_side_effects=True),
        cost_estimate=pl.CostEstimate(flops=6_000_000_000, bytes_accessed=14 << 20, transcendentals=0),
        name=f"project{index}",
    )(h, wq_t, cos_t, sin_t, wg, wu, wd)


def solution(mesh):
    n_dev = mesh.size

    def device_fn(tokens, lengths, embedding, ln_scale, w_q, w_kv, w_o, w_gate, w_up, w_down, final_scale, k_cache, v_cache):
        rank = lax.axis_index('tp')
        steps, batch = tokens.shape
        vocab_local, dim = embedding.shape
        layers, seqs, seq_len, head_dim = k_cache.shape
        heads_local = w_q.shape[2]
        width = heads_local * head_dim
        rows = steps * batch
        half = head_dim // 2
        kc = jnp.swapaxes(k_cache, 2, 3)
        vc = jnp.swapaxes(v_cache, 2, 3)
        local_len = lax.dynamic_slice_in_dim(lengths, rank * seqs, seqs)

        def by_device(per_step):
            return per_step.reshape(steps, n_dev, seqs).transpose(1, 0, 2).reshape(rows)

        tok = by_device(tokens)
        positions = by_device(lengths[None, :] + jnp.arange(steps, dtype=jnp.int32)[:, None])
        inv_freq = 10000.0 ** (-jnp.arange(half, dtype=F32) / half)
        ang = inv_freq[:, None] * positions[None, :].astype(F32)
        cos_t = jnp.cos(ang)
        sin_t = jnp.sin(ang)
        local_rows = steps * seqs
        cos_k = lax.dynamic_slice_in_dim(cos_t, rank * local_rows, local_rows, axis=1)
        sin_k = lax.dynamic_slice_in_dim(sin_t, rank * local_rows, local_rows, axis=1)
        wq_t = jnp.moveaxis(w_q, 1, 3).reshape(layers, width, dim)
        wkv_t = jnp.swapaxes(w_kv, 1, 2)
        gains = [ln_scale[l][None] for l in range(layers)] + [final_scale[None]]

        onehot = (tok[:, None] - rank * vocab_local == jnp.arange(vocab_local, dtype=jnp.int32)[None, :]).astype(BF16)
        emb = jnp.dot(onehot, embedding, preferred_element_type=F32).astype(BF16)
        x, h, k_new, v_new = boundary(n_dev, "embed", 0, (emb,), gains[0], (wkv_t[0], cos_k, sin_k), rows)
        outs = None
        for l in range(layers):
            q_seq, mlp = project(n_dev, 1 + 2 * l, h, wq_t[l], cos_t, sin_t, w_gate[l], w_up[l], w_down[l])
            o, *outs = attention(l, steps, local_len, q_seq, k_new, v_new, kc, vc, outs)
            kv_ins = (wkv_t[l + 1], cos_k, sin_k) if l + 1 < layers else None
            x, h, *kv = boundary(n_dev, "layer", 2 + 2 * l, (o, w_o[l].reshape(width, dim), mlp, x), gains[l + 1], kv_ins, rows)
            if kv:
                k_new, v_new = kv
        logits = lax.dot_general(h, embedding, (((1,), (1,)), ((), ())), preferred_element_type=F32) * dim ** -0.5
        logits = logits.reshape(n_dev, steps, seqs, vocab_local).transpose(1, 0, 2, 3).reshape(steps, batch, vocab_local)
        k_out, v_out = outs
        return logits, jnp.swapaxes(k_out, 2, 3), jnp.swapaxes(v_out, 2, 3)

    cache_spec = P(None, 'tp', None, None)
    in_specs = (P(), P(), P('tp', None), P(), P(None, None, 'tp', None), P(), P(None, 'tp', None, None), P(None, None, 'tp'), P(None, None, 'tp'), P(None, 'tp', None), P(), cache_spec, cache_spec)
    out_specs = (P(None, None, 'tp'), cache_spec, cache_spec)
    return jax.shard_map(device_fn, mesh=mesh, in_specs=in_specs, out_specs=out_specs, check_vma=False)
```

```python
import functools

import jax
import jax.numpy as jnp
from jax import lax
from jax.experimental import pallas as pl
from jax.experimental.pallas import tpu as pltpu
from jax.sharding import PartitionSpec as P

LN_EPS = 1e-6
F32 = jnp.float32
BF16 = jnp.bfloat16


def attn_kernel(layer, has_alias, steps, seqs, len_ref, q_ref, kn_ref, vn_ref, kc_ref, vc_ref, *rest):
    if has_alias:
        rest = rest[2:]
    o_ref, ko_ref, vo_ref, kbuf, vbuf, qa, qb, oa, ob, isem, osem = rest
    head_dim, seq_len = kbuf.shape[1], kbuf.shape[2]
    rows_per = steps * seqs
    srcs = q_ref.shape[0] // rows_per
    width2 = q_ref.shape[1]

    def in_copies(s):
        return (pltpu.make_async_copy(kc_ref.at[layer, s], kbuf.at[s], isem.at[0, s]),
                pltpu.make_async_copy(vc_ref.at[layer, s], vbuf.at[s], isem.at[1, s]))

    def out_copies(s):
        return (pltpu.make_async_copy(kbuf.at[s], ko_ref.at[layer, s], osem.at[0, s]),
                pltpu.make_async_copy(vbuf.at[s], vo_ref.at[layer, s], osem.at[1, s]))

    for s in range(seqs):
        for cp in in_copies(s):
            cp.start()
    qa[...] = q_ref[:, :128].astype(F32)
    qb[...] = jnp.zeros_like(qb)
    qb[:, :width2 - 128] = q_ref[:, 128:].astype(F32)
    lane = lax.broadcasted_iota(jnp.int32, (head_dim, 128), 1)
    for s in range(seqs):
        for cp in in_copies(s):
            cp.wait()
        for t in range(steps):
            p = len_ref[s] + t
            base = pl.multiple_of((p // 128) * 128, 128)
            hit = lane == (p - base)
            c = t * seqs + s
            for buf, new in ((kbuf, kn_ref), (vbuf, vn_ref)):
                tile = buf[s, :, pl.ds(base, 128)].astype(F32)
                buf[s, :, pl.ds(base, 128)] = jnp.where(hit, new[:, c:c + 1], tile).astype(BF16)
        for cp in out_copies(s):
            cp.start()

    half = lax.broadcasted_iota(jnp.int32, (steps * srcs, width2), 1) < head_dim
    n_rows = 2 * steps * srcs
    scale = head_dim ** -0.5

    def attend(s, width):
        p = len_ref[s]
        at = [pl.ds(t * seqs + s, srcs, stride=rows_per) for t in range(steps)]
        qcat = jnp.concatenate([jnp.concatenate([qa[i, :], qb[i, :]], axis=1)[:, :width2] for i in at], axis=0)
        q2 = jnp.concatenate([jnp.where(half, qcat, 0.0), jnp.where(half, 0.0, qcat)], axis=0).astype(BF16)
        k = kbuf[s, :, 0:width]
        k2 = jnp.concatenate([k, k], axis=0)
        sc = jnp.dot(q2, k2, preferred_element_type=F32) * scale
        row = lax.broadcasted_iota(jnp.int32, (n_rows, width), 0)
        col = lax.broadcasted_iota(jnp.int32, (n_rows, width), 1)
        lim = p + lax.rem(row // srcs, steps)
        sc = jnp.where(col <= lim, sc, -jnp.inf)
        m = jnp.max(sc, axis=-1, keepdims=True)
        e = jnp.exp(sc - m)
        w = (e / jnp.sum(e, axis=-1, keepdims=True)).astype(BF16)
        v = vbuf[s, :, 0:width]
        v2 = jnp.concatenate([v, v], axis=0)
        o2 = lax.dot_general(w, v2, (((1,), (1,)), ((), ())), preferred_element_type=F32)
        o = jnp.where(half, o2[:n_rows // 2], o2[n_rows // 2:])
        o = jnp.concatenate([o, jnp.zeros((steps * srcs, 256 - width2), F32)], axis=1)
        for t in range(steps):
            oa[at[t], :] = o[t * srcs:(t + 1) * srcs, :128]
            ob[at[t], :] = o[t * srcs:(t + 1) * srcs, 128:]

    widths = [w for w in (256, 512, 1024) if w < seq_len] + [seq_len]

    @pl.loop(0, seqs)
    def _(s):
        last = len_ref[s] + (steps - 1)
        lo = 0
        for w in widths:
            @pl.when((last >= lo) & (last < w))
            def _():
                attend(s, w)
            lo = w

    o_ref[:, :128] = oa[...].astype(BF16)
    o_ref[:, 128:] = ob[:, :width2 - 128].astype(BF16)
    for s in range(seqs):
        for cp in out_copies(s):
            cp.wait()


def attention(layer, steps, local_len, q, k_new, v_new, kc, vc, outs):
    layers, seqs, head_dim, seq_len = kc.shape
    rows, width = q.shape
    any_spec = pl.BlockSpec(memory_space=pltpu.HBM)
    vm = pl.BlockSpec(memory_space=pltpu.VMEM)
    args = [local_len, q, k_new, v_new, kc, vc]
    in_specs = [pl.BlockSpec(memory_space=pltpu.SMEM), vm, vm, vm, any_spec, any_spec]
    aliases = {}
    if outs is not None:
        args += list(outs)
        in_specs += [any_spec, any_spec]
        aliases = {6: 1, 7: 2}
    return pl.pallas_call(
        functools.partial(attn_kernel, layer, outs is not None, steps, seqs),
        out_shape=(jax.ShapeDtypeStruct((rows, width), BF16), jax.ShapeDtypeStruct(kc.shape, BF16), jax.ShapeDtypeStruct(vc.shape, BF16)),
        in_specs=in_specs,
        out_specs=(vm, any_spec, any_spec),
        scratch_shapes=[
            pltpu.VMEM((seqs, head_dim, seq_len), BF16),
            pltpu.VMEM((seqs, head_dim, seq_len), BF16),
            pltpu.VMEM((rows, 128), F32),
            pltpu.VMEM((rows, 128), F32),
            pltpu.VMEM((rows, 128), F32),
            pltpu.VMEM((rows, 128), F32),
            pltpu.SemaphoreType.DMA((2, seqs)),
            pltpu.SemaphoreType.DMA((2, seqs)),
        ],
        input_output_aliases=aliases,
        compiler_params=pltpu.CompilerParams(vmem_limit_bytes=24 << 20),
        cost_estimate=pl.CostEstimate(flops=2_000_000_000, bytes_accessed=21 << 20, transcendentals=1 << 20),
        name=f"attend{layer}",
    )(*args)


def device(d):
    return {"device_id": (d,), "device_id_type": pl.DeviceIdType.MESH}


def enter(n_dev, me):
    sem = pltpu.get_barrier_semaphore()
    for i in range(1, n_dev):
        pl.semaphore_signal(sem, inc=1, **device(lax.rem(me + i, n_dev)))
    return sem


def chip_at(chip, j, n_bits):
    total = 0
    for i in range(n_bits):
        total = total + lax.rem(chip // (1 << i) + ((j >> i) & 1), 2) * (1 << i)
    return total


def block(d, rows):
    return pl.ds(pl.multiple_of(d * rows, rows), rows)


def norm_rows(x_f32, gain):
    row_mean = jnp.mean(x_f32, axis=-1, keepdims=True)
    centred = x_f32 - row_mean
    row_var = jnp.mean(centred * centred, axis=-1, keepdims=True)
    return (centred * lax.rsqrt(row_var + LN_EPS) * gain).astype(BF16)


def reduce_gather(n_dev, me, part, x_ref, gain, x_out, h_out, hloc, d2d, stage, rem, sems, while_gathering):
    d2d_s, d2d_r, far_s, far_r, ag_s, ag_r, fw_s, fw_r = sems
    n_chips = n_dev // 2
    n_bits = n_chips.bit_length() - 1
    rows = hloc.shape[0]
    chip, core = me // 2, lax.rem(me, 2)
    sibling = chip * 2 + 1 - core
    order = sorted(range(n_chips), key=lambda j: -bin(j).count("1"))

    def pre(j):
        c = chip_at(chip, j, n_bits)
        return pltpu.make_async_remote_copy(part.at[block(c * 2 + 1 - core, rows)], d2d.at[j], d2d_s.at[j], d2d_r.at[j], **device(sibling))

    def far(j):
        c = chip_at(chip, j, n_bits)
        return pltpu.make_async_remote_copy(stage.at[j], rem.at[j], far_s.at[j], far_r.at[j], **device(c * 2 + core))

    for j in order:
        pre(j).start()
    for j in order[:-1]:
        pre(j).wait_recv()
        c = chip_at(chip, j, n_bits)
        stage[j] = (part[block(c * 2 + core, rows)].astype(F32) + d2d[j].astype(F32)).astype(stage.dtype)
        far(j).start()
    pre(0).wait_recv()
    acc = part[block(me, rows)].astype(F32) + d2d[0].astype(F32)
    for j in reversed(order[:-1]):
        far(j).wait_recv()
        acc = acc + rem[j].astype(F32)
    if x_ref is not None:
        acc = x_ref[...].astype(F32) + acc
    x_new = acc.astype(BF16)
    if x_out is not None:
        x_out[...] = x_new
    hloc[...] = norm_rows(x_new.astype(F32), gain)
    h_out[block(me, rows)] = hloc[...]

    def gather(j):
        c = chip_at(chip, j, n_bits)
        return pltpu.make_async_remote_copy(hloc, h_out.at[block(me, rows)], ag_s.at[j], ag_r.at[j], **device(c * 2 + core if j else sibling))

    def relay(j):
        c = chip_at(chip, j, n_bits)
        blk = h_out.at[block(c * 2 + core, rows)]
        return pltpu.make_async_remote_copy(blk, blk, fw_s.at[j], fw_r.at[j], **device(sibling))

    for j in order:
        gather(j).start()
    while_gathering()
    for j in reversed(order[:-1]):
        gather(j).wait_recv()
        relay(j).start()
    gather(0).wait_recv()
    for j in order[:-1]:
        relay(j).wait_recv()
    for j in order:
        pre(j).wait_send()
        gather(j).wait_send()
        if j:
            far(j).wait_send()
            relay(j).wait_send()


def reduce_scratch(n_dev, rows, dim, dtype):
    n_chips = n_dev // 2
    return [pltpu.VMEM((rows, dim), BF16)] + [pltpu.VMEM((n_chips, rows, dim), dtype)] * 3 + [pltpu.SemaphoreType.DMA((n_chips,))] * 8


def lookup_kernel(tok_ref, emb_ref, out_ref, buf, row32, out32, sem):
    n_rows, group = buf.shape[0], buf.shape[1]
    vocab = emb_ref.shape[0]

    def fetch(i):
        first = pl.multiple_of((tok_ref[i] // group) * group, group)
        return pltpu.make_async_copy(emb_ref.at[pl.ds(first, group), :], buf.at[i], sem.at[i])

    def each(fn):
        @pl.loop(0, n_rows // 8)
        def _(base):
            for u in range(8):
                i = base * 8 + u
                tok = tok_ref[i]

                @pl.when((tok >= 0) & (tok < vocab))
                def _():
                    fn(i, tok)

    each(lambda i, tok: fetch(i).start())
    out32[...] = jnp.zeros_like(out32)

    def place(i, tok):
        fetch(i).wait()
        row32[...] = buf[i].astype(F32)
        out32[pl.ds(i, 1), :] = row32[pl.ds(lax.rem(tok, group), 1), :]

    each(place)
    out_ref[...] = out32[...].astype(BF16)


def lookup(tok, embedding):
    rows, dim, group = tok.shape[0], embedding.shape[1], 16
    return pl.pallas_call(
        lookup_kernel,
        out_shape=jax.ShapeDtypeStruct((rows, dim), BF16),
        in_specs=[pl.BlockSpec(memory_space=pltpu.SMEM), pl.BlockSpec(memory_space=pltpu.HBM)],
        out_specs=pl.BlockSpec(memory_space=pltpu.VMEM),
        scratch_shapes=[pltpu.VMEM((rows, group, dim), BF16), pltpu.VMEM((group, dim), F32), pltpu.VMEM((rows, dim), F32), pltpu.SemaphoreType.DMA((rows,))],
        compiler_params=pltpu.CompilerParams(vmem_limit_bytes=32 << 20),
        cost_estimate=pl.CostEstimate(flops=1_000_000_000, bytes_accessed=2 << 20, transcendentals=0),
        name="lookup",
    )(tok, embedding)


def logits_kernel(n_dev, seqs, scale, h_ref, e_ref, out_ref):
    steps = out_ref.shape[0]
    acc = lax.dot_general(h_ref[...], e_ref[...], (((1,), (1,)), ((), ())), preferred_element_type=F32) * scale
    for d in range(n_dev):
        for t in range(steps):
            at = (d * steps + t) * seqs
            out_ref[t, d * seqs:(d + 1) * seqs, :] = acc[at:at + seqs]


def output_head(n_dev, steps, seqs, h, embedding):
    rows, dim = h.shape
    vocab = embedding.shape[0]
    tile = 640
    return pl.pallas_call(
        functools.partial(logits_kernel, n_dev, seqs, dim ** -0.5),
        grid=(vocab // tile,),
        out_shape=jax.ShapeDtypeStruct((steps, rows // steps, vocab), F32),
        in_specs=[pl.BlockSpec((rows, dim), lambda i: (0, 0)), pl.BlockSpec((tile, dim), lambda i: (i, 0))],
        out_specs=pl.BlockSpec((steps, rows // steps, tile), lambda i: (0, 0, i)),
        compiler_params=pltpu.CompilerParams(vmem_limit_bytes=28 << 20),
        cost_estimate=pl.CostEstimate(flops=4_000_000_000, bytes_accessed=20 << 20, transcendentals=0),
        name="head",
    )(h, embedding)


def layer_kernel(n_dev, layer, first, last, *refs):
    refs = list(refs)
    take = lambda n: [refs.pop(0) for _ in range(n)]
    if first:
        part, gain = take(2)
        x_ref = None
    else:
        o_ref, hid_ref, x_ref, gain, wo_hbm, wd_hbm = take(6)
    if not last:
        cos_ref, sin_ref, cosk_ref, sink_ref, wkv_hbm, wq_hbm, wg_hbm, wu_hbm = take(8)
        x_out, q_out, hid_out, kn_ref, vn_ref = take(5)
    else:
        (h_out,) = take(1)
    hloc, d2d, stage, rem, *sems = take(12)
    copies = []
    if not first:
        heads, part, wo, wd, a2a_s, a2a_r, w_sem = take(7)
        copies += [pltpu.make_async_copy(wd_hbm.at[layer - 1], wd, w_sem.at[0]), pltpu.make_async_copy(wo_hbm.at[layer - 1], wo, w_sem.at[1])]
    if not last:
        h_out, q_buf, wkv, wq, wg, wu, q_s, q_r, p_sem = take(9)
        starts = [pltpu.make_async_copy(src.at[layer], dst, p_sem.at[i]) for i, (src, dst) in enumerate(((wkv_hbm, wkv), (wq_hbm, wq), (wg_hbm, wg), (wu_hbm, wu)))]
    else:
        starts = []
        x_out = None
    for cp in copies + starts:
        cp.start()
    me = lax.axis_index("tp")
    bar = enter(n_dev, me)
    pl.semaphore_wait(bar, n_dev - 1)
    rows = hloc.shape[0]

    def exchange(src, dst, s_sem, r_sem):
        def send(i):
            d = lax.rem(me + i, n_dev)
            return pltpu.make_async_remote_copy(src.at[block(d, rows)], dst.at[block(me, rows)], s_sem.at[i], r_sem.at[i], **device(d))
        return [send(i) for i in range(1, n_dev)]

    if not first:
        sends = exchange(o_ref, heads, a2a_s, a2a_r)
        for cp in sends:
            cp.start()
        heads[block(me, rows)] = o_ref[block(me, rows)]
        copies[0].wait()
        part[...] = jnp.dot(hid_ref[...], wd[...], preferred_element_type=F32)
        copies[1].wait()
        for cp in sends:
            cp.wait_recv()
        part[...] = jnp.dot(heads[...], wo[...], preferred_element_type=F32) + part[...]

    def project_kv():
        head_dim = kn_ref.shape[0]
        half = head_dim // 2
        starts[0].wait()
        kv = lax.dot_general(wkv[...], hloc[...], (((1,), (1,)), ((), ())), preferred_element_type=F32)
        k_lo, k_hi = kv[:half], kv[half:head_dim]
        cos, sin = cosk_ref[...], sink_ref[...]
        kn_ref[...] = jnp.concatenate([k_lo * cos - k_hi * sin, k_lo * sin + k_hi * cos], axis=0).astype(BF16).astype(F32)
        vn_ref[...] = kv[head_dim:].astype(BF16).astype(F32)

    reduce_gather(n_dev, me, part, x_ref, gain[...], x_out, h_out, hloc, d2d, stage, rem, sems, (lambda: None) if last else project_kv)
    if not last:
        h = h_out[...]
        half = cos_ref.shape[0]
        starts[1].wait()
        qt = lax.dot_general(wq[...], h, (((1,), (1,)), ((), ())), preferred_element_type=F32)
        cos, sin = cos_ref[...], sin_ref[...]
        turned = []
        for a in range(0, qt.shape[0], 2 * half):
            lo, hi = qt[a:a + half], qt[a + half:a + 2 * half]
            turned += [lo * cos - hi * sin, lo * sin + hi * cos]
        q_buf[...] = jnp.concatenate(turned, axis=0).T.astype(BF16)
        q_sends = exchange(q_buf, q_out, q_s, q_r)
        for cp in q_sends:
            cp.start()
        q_out[block(me, rows)] = q_buf[block(me, rows)]
        starts[2].wait()
        starts[3].wait()
        gate = jnp.dot(h, wg[...], preferred_element_type=F32)
        up = jnp.dot(h, wu[...], preferred_element_type=F32)
        hid_out[...] = (gate * jax.nn.sigmoid(gate) * up).astype(BF16)
        for cp in q_sends:
            cp.wait_recv()
        for cp in q_sends:
            cp.wait_send()
    if not first:
        for cp in sends:
            cp.wait_send()


def layer_step(n_dev, layer, ins, gain, proj, rows_total):
    vm = pl.BlockSpec(memory_space=pltpu.VMEM)
    hbm = pl.BlockSpec(memory_space=pltpu.HBM)
    first, last = len(ins) == 1, proj is None
    dim = gain.shape[1]
    rows = rows_total // n_dev
    dma = pltpu.SemaphoreType.DMA
    args = list(ins[:3]) + [gain] + list(ins[3:])
    in_specs = [vm] * (2 if first else 4) + [hbm] * (0 if first else 2)
    scratch = reduce_scratch(n_dev, rows, dim, BF16 if first else F32)
    if not first:
        width, hidden = ins[0].shape[1], ins[1].shape[1]
        scratch += [pltpu.VMEM((rows_total, width), BF16), pltpu.VMEM((rows_total, dim), F32), pltpu.VMEM((width, dim), BF16), pltpu.VMEM((hidden, dim), BF16),
                    dma((n_dev,)), dma((n_dev,)), dma((2,))]
    if last:
        out_shape = (jax.ShapeDtypeStruct((rows_total, dim), BF16),)
    else:
        cos_t, sin_t, cos_k, sin_k, wkv_t, wq_t, w_gate, w_up = proj
        args += list(proj)
        in_specs += [vm] * 4 + [hbm] * 4
        width, hidden, kv = wq_t.shape[1], w_gate.shape[2], wkv_t.shape[1]
        out_shape = (jax.ShapeDtypeStruct((rows, dim), BF16), jax.ShapeDtypeStruct((rows_total, width), BF16), jax.ShapeDtypeStruct((rows_total, hidden), BF16),
                     jax.ShapeDtypeStruct((kv // 2, rows), F32), jax.ShapeDtypeStruct((kv // 2, rows), F32))
        scratch += [pltpu.VMEM((rows_total, dim), BF16), pltpu.VMEM((rows_total, width), BF16), pltpu.VMEM((kv, dim), BF16), pltpu.VMEM((width, dim), BF16),
                    pltpu.VMEM((dim, hidden), BF16), pltpu.VMEM((dim, hidden), BF16), dma((n_dev,)), dma((n_dev,)), dma((4,))]
    return pl.pallas_call(
        functools.partial(layer_kernel, n_dev, layer, first, last),
        out_shape=out_shape,
        in_specs=in_specs,
        out_specs=tuple([vm] * len(out_shape)),
        scratch_shapes=scratch,
        compiler_params=pltpu.CompilerParams(vmem_limit_bytes=40 << 20, collective_id=layer, has_side_effects=True),
        cost_estimate=pl.CostEstimate(flops=20_000_000_000, bytes_accessed=16 << 20, transcendentals=0),
        name=f"layer{layer}",
    )(*args)


def solution(mesh):
    n_dev = mesh.size

    def device_fn(tokens, lengths, embedding, ln_scale, w_q, w_kv, w_o, w_gate, w_up, w_down, final_scale, k_cache, v_cache):
        rank = lax.axis_index('tp')
        steps, batch = tokens.shape
        vocab_local, dim = embedding.shape
        layers, seqs, seq_len, head_dim = k_cache.shape
        heads_local = w_q.shape[2]
        width = heads_local * head_dim
        rows = steps * batch
        half = head_dim // 2
        kc = jnp.swapaxes(k_cache, 2, 3)
        vc = jnp.swapaxes(v_cache, 2, 3)
        local_len = lax.dynamic_slice_in_dim(lengths, rank * seqs, seqs)

        def by_device(per_step):
            return per_step.reshape(steps, n_dev, seqs).transpose(1, 0, 2).reshape(rows)

        tok = by_device(tokens)
        positions = by_device(lengths[None, :] + jnp.arange(steps, dtype=jnp.int32)[:, None])
        inv_freq = 10000.0 ** (-jnp.arange(half, dtype=F32) / half)
        ang = inv_freq[:, None] * positions[None, :].astype(F32)
        cos_t = jnp.cos(ang)
        sin_t = jnp.sin(ang)
        pos_k = (local_len[None, :] + jnp.arange(steps, dtype=jnp.int32)[:, None]).reshape(1, steps * seqs)
        ang_k = inv_freq[:, None] * pos_k.astype(F32)
        wq_t = jnp.moveaxis(w_q, 1, 3).reshape(layers, width, dim)
        wkv_t = jnp.swapaxes(w_kv, 1, 2)
        wo_r = w_o.reshape(layers, width, dim)
        proj = (cos_t, sin_t, jnp.cos(ang_k), jnp.sin(ang_k), wkv_t, wq_t, w_gate, w_up)
        gains = [ln_scale[l][None] for l in range(layers)] + [final_scale[None]]

        emb = lookup(tok - rank * vocab_local, embedding)
        x, q_seq, hid, k_new, v_new = layer_step(n_dev, 0, (emb,), gains[0], proj, rows)
        outs = None
        for l in range(layers):
            o, *outs = attention(l, steps, local_len, q_seq, k_new, v_new, kc, vc, outs)
            ins = (o, hid, x, wo_r, w_down)
            if l + 1 < layers:
                x, q_seq, hid, k_new, v_new = layer_step(n_dev, l + 1, ins, gains[l + 1], proj, rows)
            else:
                (h,) = layer_step(n_dev, l + 1, ins, gains[l + 1], None, rows)
        logits = output_head(n_dev, steps, seqs, h, embedding)
        k_out, v_out = outs
        return logits, jnp.swapaxes(k_out, 2, 3), jnp.swapaxes(v_out, 2, 3)

    cache_spec = P(None, 'tp', None, None)
    in_specs = (P(), P(), P('tp', None), P(), P(None, None, 'tp', None), P(), P(None, 'tp', None, None), P(None, None, 'tp'), P(None, None, 'tp'), P(None, 'tp', None), P(), cache_spec, cache_spec)
    out_specs = (P(None, None, 'tp'), cache_spec, cache_spec)
    return jax.shard_map(device_fn, mesh=mesh, in_specs=in_specs, out_specs=out_specs, check_vma=False)
```

```python
import functools

import jax
import jax.numpy as jnp
from jax import lax
from jax.experimental import pallas as pl
from jax.experimental.pallas import tpu as pltpu
from jax.sharding import PartitionSpec as P

LN_EPS = 1e-6
F32 = jnp.float32
BF16 = jnp.bfloat16
BIG_VMEM = 62 * 1024 * 1024 + 512 * 1024


def attn_kernel(layer, has_alias, steps, seqs, len_ref, q_ref, kn_ref, vn_ref, kc_ref, vc_ref, *rest):
    if has_alias:
        rest = rest[2:]
    o_ref, ko_ref, vo_ref, kbuf, vbuf, wide, qa, qb, oa, ob, isem, osem = rest
    head_dim, seq_len = kbuf.shape[1], kbuf.shape[2]
    rows_per = steps * seqs
    srcs = q_ref.shape[0] // rows_per
    width2 = q_ref.shape[1]

    def in_copies(s):
        return (pltpu.make_async_copy(kc_ref.at[layer, s], kbuf.at[s], isem.at[0, s]),
                pltpu.make_async_copy(vc_ref.at[layer, s], vbuf.at[s], isem.at[1, s]))

    def out_copies(s):
        return (pltpu.make_async_copy(kbuf.at[s], ko_ref.at[layer, s], osem.at[0, s]),
                pltpu.make_async_copy(vbuf.at[s], vo_ref.at[layer, s], osem.at[1, s]))

    for s in range(seqs):
        for cp in in_copies(s):
            cp.start()
    qa[...] = q_ref[:, :128].astype(F32)
    qb[...] = jnp.zeros_like(qb)
    qb[:, :width2 - 128] = q_ref[:, 128:].astype(F32)
    lane = lax.broadcasted_iota(jnp.int32, (head_dim, 128), 1)
    for c in range(rows_per):
        for i, new in enumerate((kn_ref, vn_ref)):
            wide[i, c] = jnp.broadcast_to(new[:, c:c + 1], (head_dim, 128))
    first = lax.axis_index("tp") * seqs

    def update(s):
        for cp in in_copies(s):
            cp.wait()
        for t in range(steps):
            p = len_ref[first + s] + t
            base = pl.multiple_of((p // 128) * 128, 128)
            hit = lane == (p - base)
            for i, buf in enumerate((kbuf, vbuf)):
                tile = buf[s, :, pl.ds(base, 128)].astype(F32)
                buf[s, :, pl.ds(base, 128)] = jnp.where(hit, wide[i, t * seqs + s], tile).astype(BF16)
        for cp in out_copies(s):
            cp.start()

    half = lax.broadcasted_iota(jnp.int32, (steps * srcs, width2), 1) < head_dim
    n_rows = 2 * steps * srcs
    scale = head_dim ** -0.5

    def attend(s, width):
        p = len_ref[first + s]
        at = [pl.ds(t * seqs + s, srcs, stride=rows_per) for t in range(steps)]
        qcat = jnp.concatenate([jnp.concatenate([qa[i, :], qb[i, :]], axis=1)[:, :width2] for i in at], axis=0)
        q2 = jnp.concatenate([jnp.where(half, qcat, 0.0), jnp.where(half, 0.0, qcat)], axis=0).astype(BF16)
        k = kbuf[s, :, 0:width]
        k2 = jnp.concatenate([k, k], axis=0)
        sc = jnp.dot(q2, k2, preferred_element_type=F32) * scale
        row = lax.broadcasted_iota(jnp.int32, (n_rows, width), 0)
        col = lax.broadcasted_iota(jnp.int32, (n_rows, width), 1)
        lim = p + lax.rem(row // srcs, steps)
        sc = jnp.where(col <= lim, sc, -jnp.inf)
        m = jnp.max(sc, axis=-1, keepdims=True)
        e = jnp.exp(sc - m)
        w = (e / jnp.sum(e, axis=-1, keepdims=True)).astype(BF16)
        v = vbuf[s, :, 0:width]
        v2 = jnp.concatenate([v, v], axis=0)
        o2 = lax.dot_general(w, v2, (((1,), (1,)), ((), ())), preferred_element_type=F32)
        o = jnp.where(half, o2[:n_rows // 2], o2[n_rows // 2:])
        o = jnp.concatenate([o, jnp.zeros((steps * srcs, 256 - width2), F32)], axis=1)
        for t in range(steps):
            oa[at[t], :] = o[t * srcs:(t + 1) * srcs, :128]
            ob[at[t], :] = o[t * srcs:(t + 1) * srcs, 128:]

    widths = [w for w in (256, 512, 1024) if w < seq_len] + [seq_len]

    @pl.loop(0, seqs)
    def _(s):
        update(s)
        last = len_ref[first + s] + (steps - 1)
        lo = 0
        for w in widths:
            @pl.when((last >= lo) & (last < w))
            def _():
                attend(s, w)
            lo = w

    o_ref[:, :128] = oa[...].astype(BF16)
    o_ref[:, 128:] = ob[:, :width2 - 128].astype(BF16)
    for s in range(seqs):
        for cp in out_copies(s):
            cp.wait()


def attention(layer, steps, lengths, q, k_new, v_new, kc, vc, outs):
    layers, seqs, head_dim, seq_len = kc.shape
    rows, width = q.shape
    any_spec = pl.BlockSpec(memory_space=pltpu.HBM)
    vm = pl.BlockSpec(memory_space=pltpu.VMEM)
    args = [lengths, q, k_new, v_new, kc, vc]
    in_specs = [pl.BlockSpec(memory_space=pltpu.SMEM), vm, vm, vm, any_spec, any_spec]
    aliases = {}
    if outs is not None:
        args += list(outs)
        in_specs += [any_spec, any_spec]
        aliases = {6: 1, 7: 2}
    return pl.pallas_call(
        functools.partial(attn_kernel, layer, outs is not None, steps, seqs),
        out_shape=(jax.ShapeDtypeStruct((rows, width), BF16), jax.ShapeDtypeStruct(kc.shape, BF16), jax.ShapeDtypeStruct(vc.shape, BF16)),
        in_specs=in_specs,
        out_specs=(vm, any_spec, any_spec),
        scratch_shapes=[
            pltpu.VMEM((seqs, head_dim, seq_len), BF16),
            pltpu.VMEM((seqs, head_dim, seq_len), BF16),
            pltpu.VMEM((2, steps * seqs, head_dim, 128), F32),
            pltpu.VMEM((rows, 128), F32),
            pltpu.VMEM((rows, 128), F32),
            pltpu.VMEM((rows, 128), F32),
            pltpu.VMEM((rows, 128), F32),
            pltpu.SemaphoreType.DMA((2, seqs)),
            pltpu.SemaphoreType.DMA((2, seqs)),
        ],
        input_output_aliases=aliases,
        compiler_params=pltpu.CompilerParams(vmem_limit_bytes=BIG_VMEM),
        cost_estimate=pl.CostEstimate(flops=2_000_000_000, bytes_accessed=21 << 20, transcendentals=1 << 20),
        name=f"attend{layer}",
    )(*args)


def device(d):
    return {"device_id": (d,), "device_id_type": pl.DeviceIdType.MESH}


def enter(n_dev, me):
    sem = pltpu.get_barrier_semaphore()
    for i in range(1, n_dev):
        pl.semaphore_signal(sem, inc=1, **device(lax.rem(me + i, n_dev)))
    return sem


def chip_at(chip, j, n_bits):
    total = 0
    for i in range(n_bits):
        total = total + lax.rem(chip // (1 << i) + ((j >> i) & 1), 2) * (1 << i)
    return total


def block(d, rows):
    return pl.ds(pl.multiple_of(d * rows, rows), rows)


def norm_rows(x_f32, gain):
    row_mean = jnp.mean(x_f32, axis=-1, keepdims=True)
    centred = x_f32 - row_mean
    row_var = jnp.mean(centred * centred, axis=-1, keepdims=True)
    return (centred * lax.rsqrt(row_var + LN_EPS) * gain).astype(BF16)


def column_groups(dim):
    tiles = dim // 128
    cuts = [0] + [128 * ((tiles * (i + 1) + 2) // 3) for i in range(3)]
    return [pl.ds(lo, hi - lo) for lo, hi in zip(cuts[:-1], cuts[1:])]


def reduce_gather(n_dev, me, part, x_ref, gain, x_out, h_out, hloc, d2d, acc, r1, r2, r3, sems, while_gathering):
    d2d_s, d2d_r, s1, q1, s2, q2, s3, q3, ag_s, ag_r, fw_s, fw_r = sems
    n_chips = n_dev // 2
    rows = hloc.shape[0]
    chip, core = me // 2, lax.rem(me, 2)
    sibling = chip * 2 + 1 - core
    cols = column_groups(hloc.shape[1])
    orders = [(1, 2, 4), (2, 4, 1), (4, 1, 2)]
    by_distance = sorted(range(n_chips), key=lambda j: -bin(j).count("1"))
    where = {j: chip_at(chip, j, 3) for j in range(n_chips)}
    peer = {a: device(where[a] * 2 + core) for a in (1, 2, 4)}
    copy = pltpu.make_async_remote_copy

    def pre(j):
        return copy(part.at[block(where[j] * 2 + 1 - core, rows)], d2d.at[j], d2d_s.at[j], d2d_r.at[j], **device(sibling))

    def halve1(g, i):
        a, b, c = orders[g]
        j = (b + c, b, c, 0)[i]
        return j, copy(acc.at[j + a, :, cols[g]], r1.at[i, :, cols[g]], s1.at[g, i], q1.at[g, i], **peer[a])

    def halve2(g, i):
        a, b, c = orders[g]
        j = (c, 0)[i]
        return j, copy(acc.at[j + b, :, cols[g]], r2.at[i, :, cols[g]], s2.at[g, i], q2.at[g, i], **peer[b])

    def halve3(g):
        c = orders[g][2]
        return copy(acc.at[c, :, cols[g]], r3.at[:, cols[g]], s3.at[g], q3.at[g], **peer[c])

    def add(j, g, other):
        acc[j, :, cols[g]] = (acc[j, :, cols[g]].astype(F32) + other.astype(F32)).astype(acc.dtype)

    for j in by_distance:
        pre(j).start()
    for j in by_distance:
        pre(j).wait_recv()
        acc[j] = (part[block(where[j] * 2 + core, rows)].astype(F32) + d2d[j].astype(F32)).astype(acc.dtype)
        for g in range(3):
            for i in range(4):
                k, cp = halve1(g, i)
                if k + orders[g][0] == j:
                    cp.start()
    for i in range(4):
        for g in range(3):
            j, cp = halve1(g, i)
            cp.wait_recv()
            add(j, g, r1[i, :, cols[g]])
            if i < 2:
                halve2(g, i)[1].start()
    for g in range(3):
        j, cp = halve2(g, 0)
        cp.wait_recv()
        add(j, g, r2[0, :, cols[g]])
        halve3(g).start()
    for g in range(3):
        halve2(g, 1)[1].wait_recv()
        add(0, g, r2[1, :, cols[g]])
    for g in range(3):
        halve3(g).wait_recv()
    total = acc[0].astype(F32) + r3[...].astype(F32)
    if x_ref is not None:
        total = x_ref[...].astype(F32) + total
    x_new = total.astype(BF16)
    if x_out is not None:
        x_out[...] = x_new
    hloc[...] = norm_rows(x_new.astype(F32), gain)
    h_out[block(me, rows)] = hloc[...]

    def spread(g, j, axis):
        mine = block(where[j] * 2 + core, rows)
        src = hloc.at[:, cols[g]] if j == 0 else h_out.at[mine, cols[g]]
        return copy(src, h_out.at[mine, cols[g]], ag_s.at[g, j + axis], ag_r.at[g, j + axis], **peer[axis])

    def arrive(g, j):
        a, b, c = orders[g]
        last = c if j & c else b if j & b else a
        cp = spread(g, j - last, last)
        cp.wait_recv()
        after = {a: (b, c), b: (c,), c: ()}[last]
        for axis in after:
            spread(g, j, axis).start()
        relay(g, j).start()
        return cp

    def relay(g, j):
        blk = h_out.at[block(where[j] * 2 + core, rows), cols[g]]
        return copy(blk, blk, fw_s.at[g, j], fw_r.at[g, j], **device(sibling))

    for i in range(3):
        for g in range(3):
            spread(g, 0, orders[g][i]).start()
    own = copy(hloc, h_out.at[block(me, rows)], fw_s.at[0, 0], fw_r.at[0, 0], **device(sibling))
    own.start()
    while_gathering()
    for pick in ((0,), (1,), (0, 1), (2,), (0, 2), (1, 2), (0, 1, 2)):
        for g in range(3):
            arrive(g, sum(orders[g][i] for i in pick))
    own.wait_recv()
    for j in range(1, n_chips):
        for g in range(3):
            relay(g, j).wait_recv()
    for j in range(n_chips):
        pre(j).wait_send()
    own.wait_send()
    for g in range(3):
        for i in range(4):
            halve1(g, i)[1].wait_send()
        for i in range(2):
            halve2(g, i)[1].wait_send()
        halve3(g).wait_send()
        for j in range(1, n_chips):
            a, b, c = orders[g]
            last = c if j & c else b if j & b else a
            spread(g, j - last, last).wait_send()
            relay(g, j).wait_send()


def reduce_scratch(n_dev, rows, dim, dtype):
    n_chips = n_dev // 2
    dma = pltpu.SemaphoreType.DMA
    return ([pltpu.VMEM((rows, dim), BF16)] + [pltpu.VMEM((n_chips, rows, dim), dtype)] * 2
            + [pltpu.VMEM((4, rows, dim), dtype), pltpu.VMEM((2, rows, dim), dtype), pltpu.VMEM((rows, dim), dtype)]
            + [dma((n_chips,))] * 2 + [dma((3, 4))] * 2 + [dma((3, 2))] * 2 + [dma((3,))] * 2 + [dma((3, n_chips))] * 4)


def lookup_kernel(n_dev, tok_ref, emb_ref, out_ref, found, buf, row32, out32, sem):
    n_rows, group = buf.shape[0], buf.shape[1]
    vocab = emb_ref.shape[0]
    steps, batch = tok_ref.shape
    seqs = batch // n_dev
    first = lax.axis_index("tp") * vocab

    def scan(d, count):
        for t in range(steps):
            for s in range(seqs):
                tok = tok_ref[t, d * seqs + s] - first
                found[0, count] = (d * steps + t) * seqs + s
                found[1, count] = tok
                count = count + ((tok >= 0) & (tok < vocab)).astype(jnp.int32)
        return count

    count = lax.fori_loop(0, n_dev, scan, jnp.int32(0))

    def fetch(n):
        at = pl.multiple_of((found[1, n] // group) * group, group)
        return pltpu.make_async_copy(emb_ref.at[pl.ds(at, group), :], buf.at[n], sem.at[n])

    @pl.loop(0, count)
    def _(n):
        fetch(n).start()

    out32[...] = jnp.zeros_like(out32)

    @pl.loop(0, count)
    def _(n):
        fetch(n).wait()
        row32[...] = buf[n].astype(F32)
        out32[pl.ds(found[0, n], 1), :] = row32[pl.ds(lax.rem(found[1, n], group), 1), :]

    out_ref[...] = out32[...].astype(BF16)


def lookup(n_dev, tokens, embedding):
    rows, dim, group = tokens.size, embedding.shape[1], 16
    return pl.pallas_call(
        functools.partial(lookup_kernel, n_dev),
        out_shape=jax.ShapeDtypeStruct((rows, dim), BF16),
        in_specs=[pl.BlockSpec(memory_space=pltpu.SMEM), pl.BlockSpec(memory_space=pltpu.HBM)],
        out_specs=pl.BlockSpec(memory_space=pltpu.VMEM),
        scratch_shapes=[pltpu.SMEM((2, rows), jnp.int32), pltpu.VMEM((rows, group, dim), BF16), pltpu.VMEM((group, dim), F32), pltpu.VMEM((rows, dim), F32), pltpu.SemaphoreType.DMA((rows,))],
        compiler_params=pltpu.CompilerParams(vmem_limit_bytes=BIG_VMEM),
        cost_estimate=pl.CostEstimate(flops=1_000_000_000, bytes_accessed=2 << 20, transcendentals=0),
        name="lookup",
    )(tokens, embedding)


def logits_kernel(n_dev, seqs, scale, h_ref, e_ref, out_ref):
    steps = out_ref.shape[0]
    acc = (lax.dot_general(e_ref[...], h_ref[...], (((1,), (1,)), ((), ())), preferred_element_type=F32) * scale).T
    for d in range(n_dev):
        for t in range(steps):
            at = (d * steps + t) * seqs
            out_ref[t, d * seqs:(d + 1) * seqs, :] = acc[at:at + seqs]


def output_head(n_dev, steps, seqs, h, embedding):
    rows, dim = h.shape
    vocab = embedding.shape[0]
    tile = 640
    return pl.pallas_call(
        functools.partial(logits_kernel, n_dev, seqs, dim ** -0.5),
        grid=(vocab // tile,),
        out_shape=jax.ShapeDtypeStruct((steps, rows // steps, vocab), F32),
        in_specs=[pl.BlockSpec((rows, dim), lambda i: (0, 0)), pl.BlockSpec((tile, dim), lambda i: (i, 0))],
        out_specs=pl.BlockSpec((steps, rows // steps, tile), lambda i: (0, 0, i)),
        compiler_params=pltpu.CompilerParams(vmem_limit_bytes=BIG_VMEM),
        cost_estimate=pl.CostEstimate(flops=4_000_000_000, bytes_accessed=20 << 20, transcendentals=0),
        name="head",
    )(h, embedding)


def layer_kernel(n_dev, layer, first, last, *refs):
    refs = list(refs)
    take = lambda n: [refs.pop(0) for _ in range(n)]
    if first:
        part, gain = take(2)
        x_ref = None
    else:
        o_ref, hid_ref, x_ref, gain, wo_hbm, wd_hbm = take(6)
    if not last:
        cos_ref, sin_ref, cosk_ref, sink_ref, wkv_hbm, wq_hbm, wg_hbm, wu_hbm = take(8)
        x_out, q_out, hid_out, kn_ref, vn_ref = take(5)
    else:
        (h_out,) = take(1)
    hloc, d2d, acc, r1, r2, r3, *sems = take(18)
    copies = []
    if not first:
        heads, part, wo, wd, a2a_s, a2a_r, w_sem = take(7)
        copies += [pltpu.make_async_copy(wd_hbm.at[layer - 1], wd, w_sem.at[0]), pltpu.make_async_copy(wo_hbm.at[layer - 1], wo, w_sem.at[1])]
    if not last:
        h_out, q_buf, wkv, wq, wg, wu, q_s, q_r, p_sem = take(9)
        starts = [pltpu.make_async_copy(src.at[layer], dst, p_sem.at[i]) for i, (src, dst) in enumerate(((wkv_hbm, wkv), (wq_hbm, wq), (wg_hbm, wg), (wu_hbm, wu)))]
    else:
        starts = []
        x_out = None
    for cp in copies + starts:
        cp.start()
    me = lax.axis_index("tp")
    bar = enter(n_dev, me)
    pl.semaphore_wait(bar, n_dev - 1)
    rows = hloc.shape[0]

    def exchange(src, dst, s_sem, r_sem):
        def send(i):
            d = lax.rem(me + i, n_dev)
            return pltpu.make_async_remote_copy(src.at[block(d, rows)], dst.at[block(me, rows)], s_sem.at[i], r_sem.at[i], **device(d))
        return [send(i) for i in range(1, n_dev)]

    if not first:
        sends = exchange(o_ref, heads, a2a_s, a2a_r)
        for cp in sends:
            cp.start()
        heads[block(me, rows)] = o_ref[block(me, rows)]
        copies[0].wait()
        part[...] = jnp.dot(hid_ref[...], wd[...], preferred_element_type=F32)
        copies[1].wait()
        for cp in sends:
            cp.wait_recv()
        part[...] = jnp.dot(heads[...], wo[...], preferred_element_type=F32) + part[...]

    def project_kv():
        head_dim = kn_ref.shape[0]
        half = head_dim // 2
        starts[0].wait()
        kv = lax.dot_general(wkv[...], hloc[...], (((1,), (1,)), ((), ())), preferred_element_type=F32)
        k_lo, k_hi = kv[:half], kv[half:head_dim]
        cos, sin = cosk_ref[...], sink_ref[...]
        kn_ref[...] = jnp.concatenate([k_lo * cos - k_hi * sin, k_lo * sin + k_hi * cos], axis=0).astype(BF16).astype(F32)
        vn_ref[...] = kv[head_dim:].astype(BF16).astype(F32)

    reduce_gather(n_dev, me, part, x_ref, gain[...], x_out, h_out, hloc, d2d, acc, r1, r2, r3, sems, (lambda: None) if last else project_kv)
    if not last:
        h = h_out[...]
        half = cos_ref.shape[0]
        starts[1].wait()
        qt = lax.dot_general(wq[...], h, (((1,), (1,)), ((), ())), preferred_element_type=F32)
        cos, sin = cos_ref[...], sin_ref[...]
        turned = []
        for a in range(0, qt.shape[0], 2 * half):
            lo, hi = qt[a:a + half], qt[a + half:a + 2 * half]
            turned += [lo * cos - hi * sin, lo * sin + hi * cos]
        q_buf[...] = jnp.concatenate(turned, axis=0).T.astype(BF16)
        q_sends = exchange(q_buf, q_out, q_s, q_r)
        for cp in q_sends:
            cp.start()
        q_out[block(me, rows)] = q_buf[block(me, rows)]
        starts[2].wait()
        starts[3].wait()
        gate = jnp.dot(h, wg[...], preferred_element_type=F32)
        up = jnp.dot(h, wu[...], preferred_element_type=F32)
        hid_out[...] = (gate * jax.nn.sigmoid(gate) * up).astype(BF16)
        for cp in q_sends:
            cp.wait_recv()
        for cp in q_sends:
            cp.wait_send()
    if not first:
        for cp in sends:
            cp.wait_send()


def layer_step(n_dev, layer, ins, gain, proj, rows_total):
    vm = pl.BlockSpec(memory_space=pltpu.VMEM)
    hbm = pl.BlockSpec(memory_space=pltpu.HBM)
    first, last = len(ins) == 1, proj is None
    dim = gain.shape[1]
    rows = rows_total // n_dev
    dma = pltpu.SemaphoreType.DMA
    args = list(ins[:3]) + [gain] + list(ins[3:])
    in_specs = [vm] * (2 if first else 4) + [hbm] * (0 if first else 2)
    scratch = reduce_scratch(n_dev, rows, dim, BF16 if first else F32)
    if not first:
        width, hidden = ins[0].shape[1], ins[1].shape[1]
        scratch += [pltpu.VMEM((rows_total, width), BF16), pltpu.VMEM((rows_total, dim), F32), pltpu.VMEM((width, dim), BF16), pltpu.VMEM((hidden, dim), BF16),
                    dma((n_dev,)), dma((n_dev,)), dma((2,))]
    if last:
        out_shape = (jax.ShapeDtypeStruct((rows_total, dim), BF16),)
    else:
        cos_t, sin_t, cos_k, sin_k, wkv_t, wq_t, w_gate, w_up = proj
        args += list(proj)
        in_specs += [vm] * 4 + [hbm] * 4
        width, hidden, kv = wq_t.shape[1], w_gate.shape[2], wkv_t.shape[1]
        out_shape = (jax.ShapeDtypeStruct((rows, dim), BF16), jax.ShapeDtypeStruct((rows_total, width), BF16), jax.ShapeDtypeStruct((rows_total, hidden), BF16),
                     jax.ShapeDtypeStruct((kv // 2, rows), F32), jax.ShapeDtypeStruct((kv // 2, rows), F32))
        scratch += [pltpu.VMEM((rows_total, dim), BF16), pltpu.VMEM((rows_total, width), BF16), pltpu.VMEM((kv, dim), BF16), pltpu.VMEM((width, dim), BF16),
                    pltpu.VMEM((dim, hidden), BF16), pltpu.VMEM((dim, hidden), BF16), dma((n_dev,)), dma((n_dev,)), dma((4,))]
    return pl.pallas_call(
        functools.partial(layer_kernel, n_dev, layer, first, last),
        out_shape=out_shape,
        in_specs=in_specs,
        out_specs=tuple([vm] * len(out_shape)),
        scratch_shapes=scratch,
        compiler_params=pltpu.CompilerParams(vmem_limit_bytes=BIG_VMEM, collective_id=layer, has_side_effects=True),
        cost_estimate=pl.CostEstimate(flops=20_000_000_000, bytes_accessed=16 << 20, transcendentals=0),
        name=f"layer{layer}",
    )(*args)


def solution(mesh):
    n_dev = mesh.size

    def device_fn(tokens, lengths, embedding, ln_scale, w_q, w_kv, w_o, w_gate, w_up, w_down, final_scale, k_cache, v_cache):
        rank = lax.axis_index('tp')
        steps, batch = tokens.shape
        vocab_local, dim = embedding.shape
        layers, seqs, seq_len, head_dim = k_cache.shape
        heads_local = w_q.shape[2]
        width = heads_local * head_dim
        rows = steps * batch
        half = head_dim // 2
        kc = jnp.swapaxes(k_cache, 2, 3)
        vc = jnp.swapaxes(v_cache, 2, 3)
        local_len = lax.dynamic_slice_in_dim(lengths, rank * seqs, seqs)

        def by_device(per_step):
            return per_step.reshape(steps, n_dev, seqs).transpose(1, 0, 2).reshape(rows)

        positions = by_device(lengths[None, :] + jnp.arange(steps, dtype=jnp.int32)[:, None])
        inv_freq = 10000.0 ** (-jnp.arange(half, dtype=F32) / half)
        ang = inv_freq[:, None] * positions[None, :].astype(F32)
        cos_t = jnp.cos(ang)
        sin_t = jnp.sin(ang)
        pos_k = (local_len[None, :] + jnp.arange(steps, dtype=jnp.int32)[:, None]).reshape(1, steps * seqs)
        ang_k = inv_freq[:, None] * pos_k.astype(F32)
        wq_t = jnp.moveaxis(w_q, 1, 3).reshape(layers, width, dim)
        wkv_t = jnp.swapaxes(w_kv, 1, 2)
        wo_r = w_o.reshape(layers, width, dim)
        proj = (cos_t, sin_t, jnp.cos(ang_k), jnp.sin(ang_k), wkv_t, wq_t, w_gate, w_up)
        gains = [ln_scale[l][None] for l in range(layers)] + [final_scale[None]]

        emb = lookup(n_dev, tokens, embedding)
        x, q_seq, hid, k_new, v_new = layer_step(n_dev, 0, (emb,), gains[0], proj, rows)
        outs = None
        for l in range(layers):
            o, *outs = attention(l, steps, lengths, q_seq, k_new, v_new, kc, vc, outs)
            ins = (o, hid, x, wo_r, w_down)
            if l + 1 < layers:
                x, q_seq, hid, k_new, v_new = layer_step(n_dev, l + 1, ins, gains[l + 1], proj, rows)
            else:
                (h,) = layer_step(n_dev, l + 1, ins, gains[l + 1], None, rows)
        logits = output_head(n_dev, steps, seqs, h, embedding)
        k_out, v_out = outs
        return logits, jnp.swapaxes(k_out, 2, 3), jnp.swapaxes(v_out, 2, 3)

    cache_spec = P(None, 'tp', None, None)
    in_specs = (P(), P(), P('tp', None), P(), P(None, None, 'tp', None), P(), P(None, 'tp', None, None), P(None, None, 'tp'), P(None, None, 'tp'), P(None, 'tp', None), P(), cache_spec, cache_spec)
    out_specs = (P(None, None, 'tp'), cache_spec, cache_spec)
    return jax.shard_map(device_fn, mesh=mesh, in_specs=in_specs, out_specs=out_specs, check_vma=False)
```
